32 devices in a mesh: role: 4 (over y, x), ep: 8 (over z, core).
Axes of the slice: x: 2, y: 2, z: 4, core: 2. Of those that a mesh axis runs over, the one named last changes fastest.
Arguments:
- grad_replicas: bfloat16 [4, 2, 3, 1536, 4096], P('role', None, None, 'ep'), may hold values from -24 to 24
- master_param: float32 [2, 3, 1536, 4096], P(None, None, 'ep', 'role'), may hold values from -0.09375 to 0.09375
- momentum: float32 [2, 3, 1536, 4096], P(None, None, 'ep', 'role'), may hold values from -6 to 6
- variance: float32 [2, 3, 1536, 4096], P(None, None, 'ep', 'role'), may hold values from 0.05 to 2
- tokens: bfloat16 [512, 4096], P(('role', 'ep')), may hold values from -6 to 6
- copy_expert: int32 [8], replicated, may hold values from 0 to 1, as said below
- row_copy: int32 [512], P(('role', 'ep')), may hold values from 0 to 7, as said below
- row_weight: float32 [512], P(('role', 'ep')), may hold values from 0.25 to 4
Outputs:
- param_out: float32 [2, 3, 1536, 4096], P(None, None, 'ep', 'role')
- momentum_out: float32 [2, 3, 1536, 4096], P(None, None, 'ep', 'role')
- variance_out: float32 [2, 3, 1536, 4096], P(None, None, 'ep', 'role')
- decoded: bfloat16 [512, 4096], P(('role', 'ep'))
The draws below stay inside these ranges and needn't reach their ends.
Inputs may be any that keep to these rules, and one draw needn't show every extreme that they name: `copy_expert`: each of the 2 experts is held by three to five of the 8 copies; the same map serves every rollout group. `row_copy`: rows of one rollout group name copies of that group. At most 4 of the 16 rows of one device name the same copy.
All inputs are finite; a program needn't handle non-finite values.
Results may differ from the reference program's by a relative error of at most 0.01.
Values may be sent and summed in bfloat16 or wider, within the bound.
No kernel may reach another device: no remote copies, remote signals or barrier semaphores. Data moves between devices by JAX's collectives and lax.ppermute only.
A program may use at most 128 MiB of HBM per device.

```python
import math
import jax
import jax.numpy as jnp
from jax import lax

D = 4096
FFH = 1536
EXPERTS = 2
SLOTS = 8
ROWS_DEV = 16
ROWS = 512
N_ROLE = 4
N_EP = 8


def draw_copy_expert(key, part):
    key = jax.random.fold_in(key, 11)
    pick_key, hot_key, order_key = jax.random.split(key, 3)
    pattern = jax.random.randint(pick_key, (), 0, 2)
    ranking = jax.random.permutation(hot_key, jnp.arange(2, dtype=jnp.int32))
    even = jnp.array([0, 1, 0, 1, 0, 1, 0, 1], dtype=jnp.int32)
    skewed = ranking[jnp.array([0, 0, 0, 0, 0, 1, 1, 1], dtype=jnp.int32)]
    layout = jnp.where(pattern == 0, even, skewed).astype(jnp.int32)
    return jax.random.permutation(order_key, layout)


def draw_row_copy(key, part):
    key = jax.random.fold_in(key, 23)
    limit = ROWS_DEV // 4
    blocks = ROWS // ROWS_DEV

    def one_block(index):
        block_key = jax.random.fold_in(key, index)
        order_key, bit_key, rest_key, final_key = jax.random.split(block_key, 4)
        chosen = jax.random.permutation(order_key, jnp.arange(SLOTS, dtype=jnp.int32))
        lower = jnp.where((index % 2 == 1) & (jax.random.randint(bit_key, (), 0, 2) == 1), 1, 0)
        leading = limit - lower
        others = jnp.repeat(chosen[1:], limit)
        others = jax.random.permutation(rest_key, others)
        position = jnp.arange(ROWS_DEV, dtype=jnp.int32)
        taken = others[jnp.clip(position - leading, 0, (SLOTS - 1) * limit - 1)]
        sequence = jnp.where(position < leading, chosen[0], taken).astype(jnp.int32)
        return jax.random.permutation(final_key, sequence)
    return jax.vmap(one_block)(jnp.arange(blocks, dtype=jnp.int32)).reshape(ROWS)


def with_spikes(values, stream_key, source, target, blocks, factor):
    def block_of(axis_at):
        return (jnp.arange(values.shape[axis_at]) // (values.shape[axis_at] // blocks)).reshape((-1,) + (1,) * (values.ndim - 1 - axis_at))

    first = jax.random.permutation(stream_key, blocks)[block_of(target)]
    other_side = (block_of(target) + blocks // 2) % blocks
    return jnp.where((block_of(source) == first) | (block_of(source) == other_side), factor * values, values)


def levels(key, dims, cuts, least, high):
    def one(dim, parts):
        heights = jax.random.uniform(jax.random.fold_in(jax.random.fold_in(key, 6), dim), (parts,), jnp.float32, least / len(cuts), high / len(cuts))
        return jnp.repeat(jnp.exp(heights), dims[dim] // parts).reshape((-1,) + (1,) * (len(dims) - dim - 1))

    loudness = one(*cuts[0])
    for cut in cuts[1:]:
        loudness = loudness * one(*cut)
    return loudness


def normal_values(own_key, shape, spread, most, cuts=(), kind=jnp.bfloat16):
    entries = jax.random.normal(own_key, shape, jnp.float32) * spread
    if len(cuts) > 0:
        entries = levels(own_key, shape, cuts, -0.22, 0.18) * entries
    return jnp.clip(entries, min=-most, max=most).astype(kind)


def noise_with(rng, extent, width, reach, pieces, heavy, kind=jnp.bfloat16):
    values = width * jax.random.normal(rng, extent, jnp.float32)
    if pieces:
        values = values * levels(rng, extent, pieces, -0.22, 0.18)
    return jnp.clip(with_spikes(values, jax.random.fold_in(rng, 3), *heavy), -reach, reach).astype(kind)


def setup_inputs(seed: int = 0) -> dict:
    splits = jax.random.split(jax.random.key(seed), 9)
    return {
        "grad_replicas": noise_with(splits[0], (N_ROLE, EXPERTS, 3, FFH, D), 4.0, 24.0, ((0, 4), (3, 8)), (0, 4, 4, 2.0)),
        "master_param": normal_values(splits[1], (EXPERTS, 3, FFH, D), D ** -0.5, 0.09375, ((2, 8), (3, 4)), jnp.float32),
        "momentum": normal_values(splits[2], (EXPERTS, 3, FFH, D), 1.0, 6.0, ((2, 8), (3, 4)), jnp.float32),
        "variance": jnp.clip(jnp.exp(math.log(2.0) - 3.6888794 * jax.random.uniform(splits[3], (EXPERTS, 3, FFH, D), jnp.float32) ** levels(splits[3], (EXPERTS, 3, FFH, D), ((2, 8), (3, 4)), -0.2, 0.2)), 0.05, 2.0),
        "tokens": normal_values(splits[4], (ROWS, D), 1.0, 6.0, ((0, 32),)),
        "copy_expert": draw_copy_expert(jax.random.fold_in(splits[8], 71), 0),
        "row_copy": draw_row_copy(jax.random.fold_in(splits[8], 71), 0),
        "row_weight": jnp.clip(jnp.exp(math.log(4.0) - 2.7725887 * jax.random.uniform(splits[7], (ROWS,), jnp.float32) ** levels(splits[7], (ROWS,), ((0, 32),), -0.2, 0.2)), 0.25, 4.0),
    }


beta_one = 0.9
beta_two = 0.95
adam_eps = 1e-08
learn_rate = 0.001
decay_rate = 0.1
correct_one = 1.0 - 0.9 ** 10
correct_two = 1.0 - 0.95 ** 10

def reference(grad_replicas, master_param, momentum, variance, tokens, copy_expert, row_copy, row_weight):

    def accumulate(running, replica):
        return (running + replica.astype(jnp.float32), None)
    running, _ = lax.scan(accumulate, jnp.zeros(master_param.shape, jnp.float32), grad_replicas)
    grad_mean = running / N_ROLE
    momentum_out = beta_one * momentum + (1.0 - beta_one) * grad_mean
    variance_out = beta_two * variance + (1.0 - beta_two) * grad_mean * grad_mean
    update = momentum_out / correct_one / (jnp.sqrt(variance_out / correct_two) + adam_eps) + decay_rate * master_param
    param_out = master_param - learn_rate * update
    tiles = param_out.astype(jnp.bfloat16)
    split = N_EP // 8
    groups = N_EP // split
    piece = FFH // N_EP
    row_count = tokens.shape[0]
    row_expert = copy_expert[row_copy]
    result = jnp.zeros((row_count, D), jnp.float32)
    for expert in range(EXPERTS):
        gate = jnp.dot(tokens, tiles[expert, 0].T, preferred_element_type=jnp.float32)
        up_part = jnp.dot(tokens, tiles[expert, 1].T, preferred_element_type=jnp.float32)
        hidden = (jax.nn.silu(gate) * up_part).astype(jnp.bfloat16).reshape(row_count, groups, split, piece)
        down = tiles[expert, 2].reshape(groups, split, piece, D)
        summed = jnp.zeros((row_count, D), jnp.float32)
        for member in range(split):
            partial_value = jnp.dot(hidden[:, :, member, :].reshape(row_count, groups * piece), down[:, member].reshape(groups * piece, D), preferred_element_type=jnp.float32).astype(jnp.bfloat16)
            summed = summed + partial_value.astype(jnp.float32)
        result = result + jnp.where((row_expert == expert)[:, None], summed, jnp.zeros_like(summed))
    decoded = (row_weight[:, None] * result).astype(jnp.bfloat16)
    return (param_out, momentum_out, variance_out, decoded)
```

```python
import functools

import jax
import jax.numpy as jnp
from jax import lax
from jax.experimental import pallas as pl
from jax.experimental.pallas import tpu as pltpu
from jax.sharding import PartitionSpec as P

beta_one = 0.9
beta_two = 0.95
adam_eps = 1e-08
learn_rate = 0.001
decay_rate = 0.1
correct_one = 1.0 - 0.9**10
correct_two = 1.0 - 0.95**10

LANES = 128


def swapped(block, axis, mask):
    members = range(lax.axis_size(axis))
    return lax.ppermute(block, axis, [(i, i ^ mask) for i in members])


def bits_of(size):
    return [1 << i for i in range(size.bit_length() - 1)]


def estimate(flops, nbytes):
    return pl.CostEstimate(flops=flops, bytes_accessed=nbytes, transcendentals=0)


def halving_plan(size, order):
    kept = list(range(size))
    plan = []
    for bit in order:
        sent = [k for k in kept if k & bit]
        kept = [k for k in kept if not k & bit]
        plan.append((bit, sent, [k ^ bit for k in sent]))
    return plan


def sum_body(table, *refs):
    *sources, out = refs
    if len(sources) == 1:
        out[...] = sources[0][...]
    else:
        total = sources[0][...].astype(jnp.float32)
        for source in sources[1:]:
            total += source[...].astype(jnp.float32)
        out[...] = total.astype(out.dtype)


def split_rows(rows, parts):
    return rows // parts if rows % (16 * parts) == 0 else rows


def summed_blocks(table, grad, received, count, experts, tile, width):
    first, n_experts = experts
    hidden = grad.shape[3]
    rows = split_rows(hidden, 2)
    shape = (count, n_experts, hidden, width)
    own = pl.BlockSpec(
        (1, 1, 1, rows, width), lambda g, e, i, t: (0, first + e, tile, i, t[g])
    )
    squeezed = (None, None, rows, width)
    specs = [pl.BlockSpec((None, None, None, rows, width), own.index_map)]
    for stage in range(len(received)):
        specs.append(
            pl.BlockSpec(
                squeezed, lambda g, e, i, t, s=stage: (t[(s + 1) * count + g], e, i, 0)
            )
        )
    size = count * n_experts * hidden * width
    return pl.pallas_call(
        sum_body,
        grid_spec=pltpu.PrefetchScalarGridSpec(
            num_scalar_prefetch=1,
            grid=(count, n_experts, hidden // rows),
            in_specs=specs,
            out_specs=pl.BlockSpec(squeezed, lambda g, e, i, t: (g, e, i, 0)),
        ),
        out_shape=jax.ShapeDtypeStruct(shape, grad.dtype),
        cost_estimate=estimate(8 * size, 2 * size * (2 + len(received))),
        name="summed_blocks",
    )(table, grad, *received)


def adam_body(n_received, n_alias, replicas, table, *refs):
    sources = refs[: 1 + n_received]
    master, first, second = refs[1 + n_received : 4 + n_received]
    param_out, first_out, second_out, tile_out = refs[4 + n_received + n_alias :]
    total = sources[0][...].astype(jnp.float32)
    for source in sources[1:]:
        total += source[...].astype(jnp.float32)
    mean = total * (1.0 / replicas)
    weights = master[...]
    first_new = beta_one * first[...] + (1.0 - beta_one) * mean
    second_new = beta_two * second[...] + (1.0 - beta_two) * mean * mean
    update = (
        first_new / correct_one / (jnp.sqrt(second_new / correct_two) + adam_eps)
        + decay_rate * weights
    )
    param = weights - learn_rate * update
    param_out[...] = param
    first_out[...] = first_new
    second_out[...] = second_new
    tile_out[...] = param.astype(tile_out.dtype)


def adam_blocks(
    table, grad, received, state, outputs, tiles, replicas, experts, tile, column, width, tile_at
):
    first, n_experts = experts
    hidden = grad.shape[3]
    rows = split_rows(hidden, 4)
    specs = [
        pl.BlockSpec(
            (None, None, None, rows, width), lambda e, i, t: (0, first + e, tile, i, t[0])
        )
    ]
    for stage in range(len(received)):
        specs.append(
            pl.BlockSpec(
                (None, None, rows, width), lambda e, i, t, s=stage: (t[s + 1], e, i, 0)
            )
        )
    piece = pl.BlockSpec(
        (None, None, rows, width), lambda e, i, t: (first + e, tile, i, column)
    )
    specs += [piece] * 3
    whole = [jax.ShapeDtypeStruct(x.shape, x.dtype) for x in state]
    aliased = list(outputs)
    aliases = {1 + len(specs) + i: i for i in range(len(aliased))}
    if tile_at is None:
        tile_shape = jax.ShapeDtypeStruct((n_experts, hidden, width), jnp.bfloat16)
        tile_spec = pl.BlockSpec((None, rows, width), lambda e, i, t: (e, i, 0))
    else:
        place, total_tiles = tile_at
        all_experts = state[0].shape[0]
        tile_shape = jax.ShapeDtypeStruct(
            (all_experts, total_tiles, hidden, width), jnp.bfloat16
        )
        tile_spec = pl.BlockSpec(
            (None, None, rows, width), lambda e, i, t: (first + e, place, i, 0)
        )
        if tiles is not None:
            aliases[1 + len(specs) + len(aliased)] = 3
            aliased.append(tiles)
    specs += [pl.BlockSpec(memory_space=pl.ANY)] * len(aliased)
    size = n_experts * hidden * width
    return pl.pallas_call(
        functools.partial(adam_body, len(received), len(aliased), replicas),
        grid_spec=pltpu.PrefetchScalarGridSpec(
            num_scalar_prefetch=1,
            grid=(n_experts, hidden // rows),
            in_specs=specs,
            out_specs=[piece] * 3 + [tile_spec],
        ),
        out_shape=whole + [tile_shape],
        input_output_aliases=aliases,
        cost_estimate=estimate(60 * size, size * (26 + 2 * len(received) + 2)),
        name="adam_blocks",
    )(table, grad, *received, *state, *aliased)


def plain_call(body, outs, flops, name, *args, prefetch=None):
    specs = [pl.BlockSpec(memory_space=pltpu.VMEM)] * len(args)
    nbytes = sum(x.size * x.dtype.itemsize for x in args)
    nbytes += sum(o.size * o.dtype.itemsize for o in outs)
    operands = args
    if prefetch is not None:
        specs = [pl.BlockSpec(memory_space=pltpu.SMEM)] + specs
        operands = (prefetch,) + args
    return pl.pallas_call(
        body,
        in_specs=specs,
        out_specs=[pl.BlockSpec(memory_space=pltpu.VMEM)] * len(outs),
        out_shape=outs,
        cost_estimate=estimate(flops, nbytes),
        name=name,
    )(*operands)


def shaped(shape, dtype=jnp.bfloat16):
    return jax.ShapeDtypeStruct(shape, dtype)


def columns_body(width, table, tokens, label, *outs):
    for k, out in enumerate(outs):
        start = pl.multiple_of(table[k] * width, LANES)
        out[:, :width] = tokens[:, pl.ds(start, width)]
        out[:, width:] = label[...]


def gate_up_body(width, tokens, tiles, *outs):
    contract = (((1,), (1,)), ((), ()))
    n_experts, n_tiles, hidden, _ = tiles.shape
    for k, out in enumerate(outs):
        rows = tokens[k, :, :width]
        label = tokens[k, :, width : width + 1]
        chosen = None
        for expert in range(n_experts):
            weights = tiles[expert].reshape(n_tiles * hidden, width)
            value = lax.dot_general(rows, weights, contract, preferred_element_type=jnp.float32)
            chosen = value if chosen is None else jnp.where(label == expert, value, chosen)
        out[...] = chosen.astype(out.dtype)


def hidden_body(*refs):
    *parts, out = refs
    total = parts[0][...].astype(jnp.float32)
    for part in parts[1:]:
        total += part[...].astype(jnp.float32)
    hidden = out.shape[1]
    gate = total[:, :hidden]
    up = total[:, hidden:]
    out[...] = (gate / (1.0 + jnp.exp(-gate)) * up).astype(out.dtype)


def down_body(n_role, n_tiles, width, *refs):
    hiddens = refs[:n_role]
    tokens = refs[n_role]
    tiles = refs[n_role + 1 : n_role + 1 + n_tiles]
    kept, sent = refs[n_role + 1 + n_tiles :]
    half = kept.shape[1]
    for k in range(n_role):
        rows = hiddens[k][...]
        label = tokens[k, :, width : width + 1]
        value = None
        expert = 0
        for tile in tiles:
            for inner in range(tile.shape[0]):
                mine = jnp.where(label == expert, rows, jnp.zeros_like(rows))
                part = jnp.dot(mine, tile[inner], preferred_element_type=jnp.float32)
                value = part if value is None else value + part
                expert += 1
        kept[k] = value[:half]
        sent[k] = value[half:].astype(sent.dtype)


def spread_body(n_in, *refs):
    total = refs[0][...].astype(jnp.float32)
    for part in refs[1:n_in]:
        total += part[...].astype(jnp.float32)
    outs = refs[n_in:]
    rows = total.shape[1] // len(outs)
    for index, out in enumerate(outs):
        out[...] = total[:, index * rows : (index + 1) * rows].astype(out.dtype)


def home_body(n_in, *refs):
    total = refs[0][...].astype(jnp.float32)
    for part in refs[1:n_in]:
        total += part[...].astype(jnp.float32)
    for k, out in enumerate(refs[n_in:]):
        out[...] = total[k].astype(out.dtype)


def decoded_body(width, chunks, n_role, table, weight, *refs):
    *pieces, out = refs
    scale = weight[...]
    for index, (column, piece_width) in enumerate(chunks):
        for k in range(n_role):
            start = pl.multiple_of(table[k] * width + column, LANES)
            value = pieces[index * n_role + k][...].astype(jnp.float32)
            out[:, pl.ds(start, piece_width)] = (scale * value).astype(out.dtype)


def shards(
    grad_replicas, master_param, momentum, variance, tokens, copy_expert, row_copy, row_weight
):
    n_role = lax.axis_size("role")
    n_ep = lax.axis_size("ep")
    role = lax.axis_index("role").astype(jnp.int32)
    n_experts, _, hidden, width = master_param.shape
    row_count, model_width = tokens.shape
    state = (master_param, momentum, variance)
    relative = jnp.arange(n_role, dtype=jnp.int32) ^ role

    half = max(n_experts // 2, 1)
    groups = [(0, half)] + ([(half, n_experts - half)] if n_experts > half else [])
    role_bits = bits_of(n_role)
    plans = [
        halving_plan(n_role, order) for order in (role_bits, role_bits[::-1])[: len(groups)]
    ]
    parts = 2 if width % (2 * LANES) == 0 else 1
    chunks = [(0, 0, width), (1, 0, width)]
    chunks += [(2, i * (width // parts), width // parts) for i in range(parts)]

    def block_index(k, column, piece):
        return relative[k] * (width // piece) + column // piece

    def sum_gradient(chunk, group):
        tile, column, piece = chunks[chunk]
        plan = plans[group]
        received = []
        for stage, (bit, sent, _) in enumerate(plan):
            entries = [block_index(k, column, piece) for k in sent]
            for earlier in range(stage):
                entries += [jnp.int32(plan[earlier][2].index(k)) for k in sent]
            table = jnp.stack(entries)
            outgoing = summed_blocks(
                table, grad_replicas, received, len(sent), groups[group], tile, piece
            )
            received.append(swapped(outgoing, "role", bit))
        table = jnp.stack(
            [block_index(0, column, piece)]
            + [jnp.int32(plan[t][2].index(0)) for t in range(len(plan))]
        )
        return table, received

    slots = jnp.arange(copy_expert.shape[0], dtype=jnp.int32)
    expert = jnp.sum(
        jnp.where(row_copy[:, None] == slots[None, :], copy_expert[None, :], 0), axis=1
    )
    label = jnp.broadcast_to(expert[:, None], (row_count, LANES)).astype(jnp.bfloat16)
    extended = width + LANES
    columns = plain_call(
        functools.partial(columns_body, width),
        [shaped((row_count, extended))] * n_role,
        1,
        "columns",
        tokens,
        label,
        prefetch=relative,
    )
    arrived = [columns[0]] + [swapped(columns[k], "role", k) for k in range(1, n_role)]
    gathered = jnp.stack(arrived)
    far = [m for m in range(2, n_ep, 2)]
    gathered = jnp.concatenate(
        [gathered] + [swapped(gathered, "ep", m) for m in far], axis=1
    )
    gathered = jnp.concatenate([gathered, swapped(gathered, "ep", 1)], axis=1)
    group_rows = gathered.shape[1]

    outputs = []
    gate_up = None
    pieces = []
    hiddens = None
    for chunk, (tile, column, piece) in enumerate(chunks):
        down_tiles = []
        for group in range(len(groups)):
            table, received = sum_gradient(chunk, group)
            results = adam_blocks(
                table,
                grad_replicas,
                received,
                state,
                outputs,
                gate_up,
                float(n_role),
                groups[group],
                tile,
                column // piece,
                piece,
                (tile, 2) if tile < 2 else None,
            )
            outputs = results[:3]
            if tile < 2:
                gate_up = results[3]
            else:
                down_tiles.append(results[3])
        if tile == 1:
            partial_sums = plain_call(
                functools.partial(gate_up_body, width),
                [shaped((group_rows, 2 * hidden))] * n_role,
                4 * n_role * group_rows * hidden * width * n_experts,
                "gate_up",
                gathered,
                gate_up,
            )
            arrived = [partial_sums[0]]
            arrived += [swapped(partial_sums[k], "role", k) for k in range(1, n_role)]
            (own_hidden,) = plain_call(
                hidden_body,
                [shaped((group_rows, hidden))],
                100 * group_rows * hidden,
                "hidden",
                *arrived,
            )
            hiddens = [own_hidden]
            hiddens += [swapped(own_hidden, "role", k) for k in range(1, n_role)]
        if tile == 2:
            kept, sent = plain_call(
                functools.partial(down_body, n_role, len(down_tiles), width),
                [
                    shaped((n_role, group_rows // 2, piece), jnp.float32),
                    shaped((n_role, group_rows // 2, piece)),
                ],
                2 * n_role * group_rows * hidden * piece * n_experts,
                "down",
                *hiddens,
                gathered,
                *down_tiles,
            )
            other = swapped(sent, "ep", 1)
            count = n_ep // 2
            spread = plain_call(
                functools.partial(spread_body, 2),
                [shaped((n_role, row_count, piece))] * count,
                n_role * group_rows * piece,
                "spread",
                kept,
                other,
            )
            arrived = [spread[0]]
            arrived += [swapped(spread[i], "ep", 2 * i) for i in range(1, count)]
            home = plain_call(
                functools.partial(home_body, count),
                [shaped((row_count, piece))] * n_role,
                n_role * group_rows * piece,
                "home",
                *arrived,
            )
            pieces.append(home[0])
            pieces += [swapped(home[k], "role", k) for k in range(1, n_role)]
    (decoded,) = plain_call(
        functools.partial(
            decoded_body, width, [(c, w) for t, c, w in chunks if t == 2], n_role
        ),
        [shaped((row_count, model_width))],
        4 * row_count * model_width,
        "decoded",
        row_weight[:, None],
        *pieces,
        prefetch=relative,
    )
    return (*outputs, decoded)


def solution(mesh):
    return jax.shard_map(
        shards,
        mesh=mesh,
        in_specs=(
            P("role", None, None, "ep", None),
            P(None, None, "ep", "role"),
            P(None, None, "ep", "role"),
            P(None, None, "ep", "role"),
            P(("role", "ep"), None),
            P(),
            P(("role", "ep")),
            P(("role", "ep")),
        ),
        out_specs=(
            P(None, None, "ep", "role"),
            P(None, None, "ep", "role"),
            P(None, None, "ep", "role"),
            P(("role", "ep"), None),
        ),
        check_vma=False,
    )
```
